256 devices in a mesh: row: 32 (over x, z_lo, core), col: 8 (over z_hi, y).
Axes of the slice: x: 4, y: 4, z: 8 (z_hi: 2, z_lo: 4; z = z_hi * 4 + z_lo), core: 2. Of those that a mesh axis runs over, the one named last changes fastest.
Arguments:
- features: bfloat16 [131072, 256], P(('row', 'col')), may hold values from -6 to 6
- grad_out: bfloat16 [131072, 256], P(('row', 'col')), may hold values from -6 to 6
- weight: bfloat16 [256, 256], replicated, may hold values from -0.375 to 0.375
- tiles: bfloat16 [49152, 128, 128], P(('row', 'col')), may hold values from -0.125 to 0.125
- tile_row: int32 [49152], P(('row', 'col')), may hold values from 0 to 31
- tile_col: int32 [49152], P(('row', 'col')), may hold values from 0 to 127
- tile_count: int32 [256], P(('row', 'col')), may hold values from 24 to 192, as said below
Outputs:
- grad_features: bfloat16 [131072, 256], P(('row', 'col'))
- grad_weight: float32 [256, 256], replicated
The draws below stay inside these ranges and needn't reach their ends.
Inputs may be any that keep to these rules, and one draw needn't show every extreme that they name: `tile_count`: exactly 192 on some device in every draw; slots of a device from its count on are not part of the adjacency.
All inputs are finite; a program needn't handle non-finite values.
Results may differ from the reference program's by a relative error of at most 0.02.
Values may be sent and summed in bfloat16 or wider, within the bound.
No kernel may reach another device: no remote copies, remote signals or barrier semaphores. Data moves between devices by JAX's collectives and lax.ppermute only.
A program may use at most 128 MiB of HBM per device.

```python
import jax
import jax.numpy as jnp
from jax import lax

F = 256
TILE = 128
MAXT = 192
V = 131072
RT = 32
CT = 128
N_ROW = 32
N_COL = 8
DEVICES = 256


def draw_tile_count(key, part):
    light_load = jax.random.randint(jax.random.fold_in(key, 11), (DEVICES,), MAXT // 8, MAXT // 3 + 1)
    heavy_load = jax.random.randint(jax.random.fold_in(key, 12), (DEVICES,), MAXT // 2, MAXT + 1)
    heavy_pick = jax.random.randint(jax.random.fold_in(key, 13), (DEVICES,), 0, 8) == 0
    counts = jnp.where(heavy_pick, heavy_load, light_load)
    top_device = jax.random.randint(jax.random.fold_in(key, 14), (), 0, DEVICES)
    counts = jnp.where(jnp.arange(DEVICES, dtype=jnp.int32) == top_device, MAXT, counts)
    return counts.astype(jnp.int32)


def with_ends(drawn, stream_key, low, largest):
    spot = [jax.random.randint(jax.random.fold_in(stream_key, axis), (), 0, length) for axis, length in enumerate(drawn.shape)]
    widest = drawn.shape.index(max(drawn.shape))
    beside = spot[:widest] + [(spot[widest] + 1) % drawn.shape[widest]] + spot[widest + 1:]
    return drawn.at[tuple(spot)].set(low).at[tuple(beside)].set(largest)


def steps_of(stream_key, extent, shards, low, largest):
    gain = 1.0
    for axis_at, parts in shards:
        draws = jax.random.uniform(jax.random.fold_in(jax.random.fold_in(stream_key, 6), axis_at), (parts,), jnp.float32, low / len(shards), largest / len(shards))
        gain = gain * jnp.repeat(jnp.exp(draws), extent[axis_at] // parts).reshape((-1,) + (1,) * (len(extent) - 1 - axis_at))
    return gain


def noise(own_key, extent, deviation, bound, cuts=(), kind=jnp.bfloat16):
    result = jax.random.normal(own_key, extent, jnp.float32) * deviation
    if len(cuts) > 0:
        result = steps_of(own_key, extent, cuts, -0.22, 0.18) * result
    return jnp.clip(result, min=-bound, max=bound).astype(kind)


def setup_inputs(seed: int = 0) -> dict:
    arg_keys = jax.random.split(jax.random.key(seed), 8)
    return {
        "features": noise(arg_keys[0], (V, F), 1.0, 6.0, ((0, 256),)),
        "grad_out": noise(arg_keys[1], (V, F), 1.0, 6.0, ((0, 256),)),
        "weight": noise(arg_keys[2], (F, F), F ** -0.5, 0.375),
        "tiles": noise(arg_keys[3], (DEVICES * MAXT, TILE, TILE), (TILE * TILE // 8) ** -0.5, 0.125, ((0, 256),)),
        "tile_row": with_ends(jax.random.randint(arg_keys[4], (DEVICES * MAXT,), 0, RT), jax.random.fold_in(arg_keys[4], 1), 0, RT - 1).astype(jnp.int32),
        "tile_col": with_ends(jax.random.randint(arg_keys[5], (DEVICES * MAXT,), 0, CT), jax.random.fold_in(arg_keys[5], 1), 0, CT - 1).astype(jnp.int32),
        "tile_count": draw_tile_count(jax.random.fold_in(arg_keys[7], 71), 0),
    }


def reference(features, grad_out, weight, tiles, tile_row, tile_col, tile_count):
    devices = N_ROW * N_COL
    tile_size = tiles.shape[1]
    feat_width = weight.shape[0]
    segment = features.shape[0] // devices
    slots = tiles.shape[0] // devices
    row_tiles = N_COL * segment // tile_size
    col_tiles = N_ROW * segment // tile_size
    mixed_rows = jnp.dot(features, weight, preferred_element_type=jnp.float32).astype(jnp.bfloat16)
    panels = mixed_rows.reshape(N_ROW, N_COL, segment, feat_width).transpose(1, 0, 2, 3)
    panels = panels.reshape(N_COL, col_tiles, tile_size, feat_width)
    tile_sets = tiles.reshape(devices, slots, tile_size, tile_size)
    row_ids = tile_row.reshape(devices, slots)
    col_ids = tile_col.reshape(devices, slots)
    live_mask = (jnp.arange(slots, dtype=jnp.int32)[None, :] < tile_count[:, None]).astype(jnp.float32)

    def forward(total, device_index):
        row_index = device_index // N_COL
        col_index = device_index % N_COL
        picked = panels[col_index][col_ids[device_index]]
        product = jnp.einsum("sij,sjf->sif", tile_sets[device_index].astype(jnp.float32),
                             picked.astype(jnp.float32), precision=lax.Precision.HIGHEST)
        product = product * live_mask[device_index][:, None, None]
        return total.at[row_index, row_ids[device_index]].add(product), None

    start = jnp.zeros((N_ROW, row_tiles, tile_size, feat_width), jnp.float32)
    preact = lax.scan(forward, start, jnp.arange(devices, dtype=jnp.int32))[0]
    preact = preact.reshape(devices * segment, feat_width)
    sigmoid_z = jax.nn.sigmoid(preact)
    grad_pre = (grad_out.astype(jnp.float32) * sigmoid_z * (1.0 + preact * (1.0 - sigmoid_z))).astype(jnp.bfloat16)
    grad_blocks = grad_pre.reshape(N_ROW, row_tiles, tile_size, feat_width)

    def backward(total, device_index):
        row_index = device_index // N_COL
        col_index = device_index % N_COL
        picked = grad_blocks[row_index][row_ids[device_index]]
        product = jnp.einsum("sji,sjf->sif", tile_sets[device_index].astype(jnp.float32),
                             picked.astype(jnp.float32), precision=lax.Precision.HIGHEST)
        product = product * live_mask[device_index][:, None, None]
        part = jnp.zeros((col_tiles, tile_size, feat_width), jnp.float32).at[col_ids[device_index]].add(product)
        part = part.astype(jnp.bfloat16).astype(jnp.float32)
        return total.at[col_index].add(part), None

    start_back = jnp.zeros((N_COL, col_tiles, tile_size, feat_width), jnp.float32)
    grad_sum = lax.scan(backward, start_back, jnp.arange(devices, dtype=jnp.int32))[0]
    grad_sum = grad_sum.reshape(N_COL, N_ROW, segment, feat_width).transpose(1, 0, 2, 3)
    grad_panel = grad_sum.reshape(devices * segment, feat_width).astype(jnp.bfloat16)
    grad_features = jnp.dot(grad_panel, weight.T, preferred_element_type=jnp.float32).astype(jnp.bfloat16)
    grad_weight = jnp.dot(features.T, grad_panel, preferred_element_type=jnp.float32)
    return grad_features, grad_weight
```

```python
import functools

import jax
import jax.numpy as jnp
from jax import lax
from jax.experimental import pallas as pl
from jax.experimental.pallas import tpu as pltpu
from jax.sharding import Mesh
from jax.sharding import PartitionSpec as P

X, ZLO, CORE, ZHI, Y = "x", "z_lo", "core", "z_hi", "y"
ROW_COL = (X, ZLO, CORE, ZHI, Y)
UNROLL = 8
MIB = 1024 * 1024


def shift(x, axis, step):
    length = lax.axis_size(axis)
    return lax.ppermute(x, axis, [(i, (i + step) % length) for i in range(length)])


def plus(*terms):
    return sum(t.astype(jnp.float32) for t in terms).astype(jnp.bfloat16)


def near(axis, step):
    return lax.rem(lax.axis_index(axis) + step, lax.axis_size(axis))


def row_place(dx, dz, dcore):
    return (near(X, dx) * 4 + near(ZLO, dz)) * 2 + near(CORE, dcore)


def col_place(dzhi, dy):
    return near(ZHI, dzhi) * 4 + near(Y, dy)


def tile_products(transpose, place_in, place_out, *refs):
    count, read_ids, write_ids, tiles = refs[:4]
    parts = refs[4 : 4 + len(place_in)]
    outs = refs[4 + len(place_in) : -3]
    panel, total, arrived = refs[-3:]
    size = tiles.shape[1]
    segment = parts[0].shape[0]
    blocks = total.shape[0] // size
    contract = (((0,), (0,)), ((), ())) if transpose else (((1,), (0,)), ((), ()))

    copies = []
    for k, (part, place) in enumerate(zip(parts, place_in)):
        start = pl.multiple_of(place() * segment, segment)
        copies.append(pltpu.make_async_copy(part, panel.at[pl.ds(start, segment), :], arrived.at[k]))
        copies[-1].start()

    def rows(tile):
        return pl.ds(pl.multiple_of(tile * size, size), size)

    def clear(tile, carry):
        total[rows(tile), :] = jnp.zeros((size, total.shape[1]), jnp.float32)
        return carry

    lax.fori_loop(0, blocks, clear, 0)
    for copy in copies:
        copy.wait()

    def add(slot):
        picked = panel[rows(read_ids[slot]), :]
        product = lax.dot_general(tiles[slot], picked, contract, preferred_element_type=jnp.float32)
        total[rows(write_ids[slot]), :] += product

    def batch(step, carry):
        for k in range(UNROLL):
            add(step * UNROLL + k)
        return carry

    def single(slot, carry):
        add(slot)
        return carry

    live = count[0]
    full = lax.div(live, UNROLL)
    lax.fori_loop(0, full, batch, 0)
    lax.fori_loop(full * UNROLL, live, single, 0)

    for out, places in zip(outs, place_out):
        for k, place in enumerate(places):
            start = place() * segment

            def store(tile, carry, out=out, k=k, start=start):
                here = pl.ds(pl.multiple_of(start + tile * size, size), size)
                out[k, rows(tile), :] = total[here, :].astype(out.dtype)
                return carry

            lax.fori_loop(0, segment // size, store, 0)


def spread_tiles(tiles, read_ids, write_ids, count, parts, place_in, place_out, transpose):
    slots, size, _ = tiles.shape
    segment, width = parts[0].shape
    in_rows = segment * len(parts)
    out_rows = segment * sum(len(places) for places in place_out)
    smem = pl.BlockSpec(memory_space=pltpu.SMEM)
    vmem = pl.BlockSpec(memory_space=pltpu.VMEM)
    return pl.pallas_call(
        functools.partial(tile_products, transpose, place_in, place_out),
        out_shape=[
            jax.ShapeDtypeStruct((len(places), segment, width), jnp.bfloat16) for places in place_out
        ],
        in_specs=[smem, smem, smem, vmem] + [pl.BlockSpec(memory_space=pl.ANY)] * len(parts),
        out_specs=[vmem] * len(place_out),
        scratch_shapes=[
            pltpu.VMEM((in_rows, width), jnp.bfloat16),
            pltpu.VMEM((out_rows, width), jnp.float32),
            pltpu.SemaphoreType.DMA((len(parts),)),
        ],
        compiler_params=pltpu.CompilerParams(vmem_limit_bytes=60 * MIB),
        cost_estimate=pl.CostEstimate(
            flops=2 * slots * size * size * width,
            bytes_accessed=2 * (slots * size * size + (in_rows + out_rows) * width),
            transcendentals=0,
        ),
        name="spread_back" if transpose else "spread_fore",
    )(count, read_ids, write_ids, tiles, *parts)


def middle(*refs):
    terms, (upstream, weight, grad_mixed, grad_weight) = refs[:-4], refs[-4:]
    total = terms[0][...].astype(jnp.float32)
    for term in terms[1:]:
        total = total + term[...].astype(jnp.float32)
    gathered = total.astype(jnp.bfloat16)
    preact = jnp.dot(gathered, weight[...], preferred_element_type=jnp.float32)
    sigmoid_z = jax.nn.sigmoid(preact)
    grad_pre = upstream[...].astype(jnp.float32) * sigmoid_z * (1.0 + preact * (1.0 - sigmoid_z))
    grad_pre = grad_pre.astype(jnp.bfloat16)
    grad_mixed[...] = lax.dot_general(
        grad_pre, weight[...], (((1,), (1,)), ((), ())), preferred_element_type=jnp.float32
    ).astype(jnp.bfloat16)
    grad_weight[...] = lax.dot_general(
        gathered, grad_pre, (((0,), (0,)), ((), ())), preferred_element_type=jnp.float32
    )


def layer_turn(terms, upstream, weight):
    segment, width = upstream.shape
    vmem = pl.BlockSpec(memory_space=pltpu.VMEM)
    return pl.pallas_call(
        middle,
        out_shape=(
            jax.ShapeDtypeStruct((segment, width), jnp.bfloat16),
            jax.ShapeDtypeStruct((width, width), jnp.float32),
        ),
        in_specs=[vmem] * (len(terms) + 2),
        out_specs=(vmem, vmem),
        compiler_params=pltpu.CompilerParams(vmem_limit_bytes=24 * MIB),
        cost_estimate=pl.CostEstimate(
            flops=6 * segment * width * width,
            bytes_accessed=12 * segment * width,
            transcendentals=segment * width,
        ),
        name="layer_turn",
    )(*terms, upstream, weight)


def gather_row(own):
    level = [(own, 0)] + [(shift(own, ZLO, k), 4 - k) for k in (1, 2, 3)]
    near_items = []
    for i, (item, dz) in enumerate(level):
        right, left = shift(item, X, 1), shift(item, X, -1)
        far = shift(right, X, 1) if i in (0, 2) else shift(left, X, -1)
        near_items += [(item, 0, dz), (right, 3, dz), (left, 1, dz), (far, 2, dz)]
    parts, places = [], []
    for item, dx, dz in near_items:
        parts += [item, shift(item, CORE, 1)]
        places += [functools.partial(row_place, dx, dz, 0), functools.partial(row_place, dx, dz, 1)]
    return parts, places


def ring_sum(pieces, axis, step):
    onward, back = (1, 3) if step == 1 else (3, 1)
    passed = plus(pieces[onward], shift(pieces[2], axis, step))
    return [pieces[0], shift(passed, axis, step), shift(pieces[back], axis, -step)]


def gather_col(own):
    other = shift(own, ZHI, 1)
    parts, places = [], []
    for item, dzhi, step in ((own, 0, 1), (other, 1, -1)):
        right, left = shift(item, Y, 1), shift(item, Y, -1)
        far = shift(right, Y, 1) if step == 1 else shift(left, Y, -1)
        parts += [item, right, left, far]
        places += [functools.partial(col_place, dzhi, dy) for dy in (0, 3, 1, 2)]
    return parts, places


def own_sum(pieces, axis):
    total = lax.dynamic_index_in_dim(pieces, lax.axis_index(axis), keepdims=False)
    for step in range(1, 4):
        piece = lax.dynamic_index_in_dim(pieces, near(axis, step), keepdims=False)
        total = total + shift(piece, axis, step)
    return total


def all_pieces(piece, axis):
    whole = jnp.zeros((4, *piece.shape), piece.dtype)
    whole = lax.dynamic_update_index_in_dim(whole, piece, lax.axis_index(axis), 0)
    for step in range(1, 4):
        came = shift(piece, axis, step)
        whole = lax.dynamic_update_index_in_dim(whole, came, near(axis, 4 - step), 0)
    return whole


def sum_everywhere(x):
    shape = x.shape
    x = x.reshape(4, 4, 4, -1, 128)
    for axis in (Y, X, ZLO):
        x = own_sum(x, axis)
    x = x + shift(x, CORE, 1)
    x = x + shift(x, ZHI, 1)
    for axis in (ZLO, X, Y):
        x = all_pieces(x, axis)
    return x.reshape(shape)


def body(features, grad_out, weight, tiles, tile_row, tile_col, tile_count):
    parts, places = gather_row(features)
    far_out = [[functools.partial(col_place, dzhi, dy)] for dzhi in (1, 0) for dy in range(4)]
    pieces = spread_tiles(tiles, tile_col, tile_row, tile_count, parts, places, far_out, False)
    pieces = [piece[0] for piece in pieces]
    crossing = plus(*ring_sum(pieces[:4], Y, 1))
    terms = ring_sum(pieces[4:], Y, -1) + [shift(crossing, ZHI, 1)]
    grad_mixed, local_weight = layer_turn(terms, grad_out, weight)

    parts, places = gather_col(grad_mixed)
    order = (1, 2, 3, 0)
    back_out = [
        [functools.partial(row_place, dx, dz, dcore) for dx in range(4)] for dcore in (1, 0) for dz in order
    ]
    blocks = spread_tiles(tiles, tile_row, tile_col, tile_count, parts, places, back_out, True)
    final = []
    for dz, away, mine in zip(order, blocks[:4], blocks[4:]):
        came = shift(away, CORE, 1)
        pieces = [plus(mine[k], came[k]) for k in range(4)]
        terms = ring_sum(pieces, X, 1 if dz in (1, 3) else -1)
        final += terms if dz == 0 else [shift(plus(*terms), ZLO, dz)]
    grad_features = plus(*final)
    return (grad_features, sum_everywhere(local_weight))


def solution(mesh):
    split = Mesh(mesh.devices.reshape(4, 4, 2, 2, 4), ROW_COL)
    in_specs = (
        P(ROW_COL, None),
        P(ROW_COL, None),
        P(),
        P(ROW_COL, None, None),
        P(ROW_COL),
        P(ROW_COL),
        P(ROW_COL),
    )
    out_specs = (P(ROW_COL, None), P())
    return jax.shard_map(body, mesh=split, in_specs=in_specs, out_specs=out_specs, check_vma=False)
```
